256 devices in a mesh: virt: 2 (over y_lo), occ: 16 (over z, y_hi), aux: 8 (over x, core).
Axes of the slice: x: 4, y: 4 (y_hi: 2, y_lo: 2; y = y_hi * 2 + y_lo), z: 8, core: 2. Of those that a mesh axis runs over, the one named last changes fastest.
Arguments:
- three_index: bfloat16 [16384, 16, 1536], P('aux', 'occ', 'virt'), may hold values from -0.59765625 to 0.59765625
- occupied_energy: bfloat16 [16], P('occ'), may hold values from -2 to -0.5
- virtual_energy: float32 [1536], P('virt'), may hold values from 0.2 to 3
Outputs:
- density: bfloat16 [16384, 16, 1536], P('aux', 'occ', 'virt')
The draws below stay inside these ranges and needn't reach their ends.
All inputs are finite; a program needn't handle non-finite values.
Results may differ from the reference program's by a relative error of at most 0.0046.
Values may be sent and summed in bfloat16 or wider, within the bound.
No kernel may reach another device: no remote copies, remote signals or barrier semaphores. Data moves between devices by JAX's collectives and lax.ppermute only.
A program may use at most 64 MiB of HBM per device.

```python
import math
import jax
import jax.numpy as jnp
from jax import lax

NAUX = 16384
VS = 768
OCC_DEV = 1
NOCC = 16
NVIRT = 1536
N_VIRT = 2
N_OCC = 16


def shard_levels(stream_key, shape, cuts, smallest, high):
    level = 1.0
    for dim, parts in cuts:
        draws = jax.random.uniform(jax.random.fold_in(jax.random.fold_in(stream_key, 6), dim), (parts,), jnp.float32, smallest / len(cuts), high / len(cuts))
        level = level * jnp.repeat(jnp.exp(draws), shape[dim] // parts).reshape((-1,) + (1,) * (len(shape) - 1 - dim))
    return level


def bell_draw(rng, dims, spread, reach, shards=(), kind=jnp.bfloat16):
    level = shard_levels(rng, dims, shards, -0.22, 0.18) if shards else 1.0
    entries = jax.random.normal(rng, dims, jnp.float32) * spread * level
    return jnp.minimum(jnp.maximum(entries, -reach), reach).astype(kind)


def setup_inputs(seed: int = 0) -> dict:
    seeds = jax.random.split(jax.random.key(seed), 4)
    three_index = bell_draw(seeds[0], (NAUX, NOCC, NVIRT), 0.1, 0.59765625, ((0, 8), (1, 16), (2, 2)))
    occupied_energy = jnp.clip(-2.0 + 1.5 * jax.random.uniform(seeds[1], (NOCC,), jnp.float32) ** shard_levels(seeds[1], (NOCC,), ((0, 16),), -0.2, 0.2), -2.0, -0.5).astype(jnp.bfloat16)
    virtual_energy = jnp.clip(jnp.exp(math.log(3.0) - 2.7080502 * jax.random.uniform(seeds[2], (NVIRT,), jnp.float32) ** shard_levels(seeds[2], (NVIRT,), ((0, 2),), -0.2, 0.2)), 0.2, 3.0)
    return dict(three_index=three_index, occupied_energy=occupied_energy, virtual_energy=virtual_energy)


spin_scale = 1.2


def pair_amplitudes(left_block, right_block, left_occupied, right_occupied, virtual_slab):
    pair_sums = lax.dot_general(left_block, right_block, (((0,), (0,)), ((), ())), preferred_element_type=jnp.float32)
    left_levels = (virtual_slab[None, :] - left_occupied.astype(jnp.float32)[:, None]).reshape(-1)
    right_levels = (virtual_slab[None, :] - right_occupied.astype(jnp.float32)[:, None]).reshape(-1)
    denominator = left_levels[:, None] + right_levels[None, :]
    return (spin_scale * pair_sums / denominator).astype(jnp.bfloat16)


def reference(three_index, occupied_energy, virtual_energy):
    blocks = three_index.reshape(NAUX, N_OCC, OCC_DEV, N_VIRT, VS)
    energies = occupied_energy.reshape(N_OCC, OCC_DEV)
    results = []
    for group in range(N_VIRT):
        slab_blocks = jnp.transpose(blocks[:, :, :, group, :].reshape(NAUX, N_OCC, OCC_DEV * VS), (1, 0, 2))
        virtual_slab = virtual_energy[group * VS:(group + 1) * VS]

        def visit(position, accumulated):
            position = jnp.asarray(position).astype(jnp.int32)
            for offset in (1, 2):
                partner = ((position - offset) % N_OCC).astype(jnp.int32)
                left_block = slab_blocks[position]
                right_block = slab_blocks[partner]
                amplitude = pair_amplitudes(left_block, right_block, energies[position], energies[partner], virtual_slab)
                own_term = lax.dot_general(right_block, amplitude, (((1,), (1,)), ((), ())), preferred_element_type=jnp.float32)
                partner_term = jnp.dot(left_block, amplitude, preferred_element_type=jnp.float32)
                accumulated = accumulated.at[position].add(own_term)
                accumulated = accumulated.at[partner].add(partner_term)
            return accumulated

        accumulated = lax.fori_loop(0, N_OCC, visit, jnp.zeros((N_OCC, NAUX, OCC_DEV * VS), jnp.float32))
        rounded = accumulated.astype(jnp.bfloat16)
        results.append(jnp.transpose(rounded, (1, 0, 2)).reshape(NAUX, N_OCC, OCC_DEV, VS))
    stacked = jnp.stack(results, axis=3)
    return stacked.reshape(NAUX, N_OCC * OCC_DEV, N_VIRT * VS)
```

```python
import functools

import jax
import jax.numpy as jnp
from jax import lax
from jax.experimental import pallas as pl
from jax.experimental.pallas import tpu as pltpu
from jax.sharding import Mesh
from jax.sharding import PartitionSpec as P


SPIN_SCALE = 1.2
X, C = 4, 2
F32, BF16 = jnp.float32, jnp.bfloat16
TN = (((0,), (0,)), ((), ()))
NN = (((1,), (0,)), ((), ()))
NT = (((1,), (1,)), ((), ()))


def mm(left, right, dims):
    return lax.dot_general(left, right, dims, preferred_element_type=F32)


def ring(axis, distance):
    size = lax.axis_size(axis)
    return [(i, (i + distance) % size) for i in range(size)]


def moved(value, axis, distance):
    return lax.ppermute(value, axis, ring(axis, distance))


def after(value, *events):
    return lax.optimization_barrier((value, *events))[0]


def add_product(step, core, left, right, place, send, keep):
    n = left.shape[1]
    half = n // C
    part = half // X
    for side, out in ((1 - core, send), (core, keep)):
        columns = pl.ds(pl.multiple_of(side * half, 128), half)
        product = mm(left[:, columns], right[...], TN)

        @pl.when(step == 0)
        def _():
            for j in range(X):
                out[j, place] = product[j * part : (j + 1) * part]

        @pl.when(step != 0)
        def _():
            for j in range(X):
                out[j, place] += product[j * part : (j + 1) * part]


def far_pairs_kernel(where, own_high, ahead, behind, own_low, send, keep):
    step, core = pl.program_id(0), where[1]
    add_product(step, core, own_high, ahead, 0, send, keep)
    add_product(step, core, behind, own_low, 1, send, keep)


def near_pairs_kernel(where, own, partner, ahead, behind, send, keep):
    step, core = pl.program_id(0), where[1]

    @pl.when(where[0] == 0)
    def _():
        add_product(step, core, partner, own, 0, send, keep)
        add_product(step, core, behind, partner, 1, send, keep)

    @pl.when(where[0] == 1)
    def _():
        add_product(step, core, own, partner, 0, send, keep)
        add_product(step, core, partner, ahead, 1, send, keep)


def pair_call(kernel, where, operands, maps, half, n, name):
    depth = 256
    out = jax.ShapeDtypeStruct((X, 2, n // (X * C), n), F32)
    specs = [pl.BlockSpec((depth, n), m) for m in maps]
    whole = pl.BlockSpec(out.shape, lambda k, s: (0, 0, 0, 0))
    return pl.pallas_call(
        kernel,
        grid_spec=pltpu.PrefetchScalarGridSpec(
            num_scalar_prefetch=1,
            grid=(half // depth,),
            in_specs=specs,
            out_specs=[whole, whole],
        ),
        out_shape=[out, out],
        name=name,
        cost_estimate=pl.CostEstimate(
            flops=4 * half * n * n, bytes_accessed=8 * half * n + 8 * n * n, transcendentals=0
        ),
    )(where, *operands)


def assemble(where, pieces, full):
    part = pieces[0].shape[1]
    core, x = where[1], where[2]
    for number, piece in enumerate(pieces):
        turn, other = number % X, number // X
        row = (core + other) % C * (part * X) + (x + turn) % X * part
        for place in range(2):
            full[place, pl.ds(pl.multiple_of(row, 32), part), :] = piece[place]


def far_terms_kernel(where, *refs):
    pieces, (ahead0, ahead1, behind0, behind1, out, full) = refs[: X * C], refs[X * C :]

    @pl.when(pl.program_id(0) == 0)
    def _():
        assemble(where, pieces, full)

    for place, (ahead, behind) in enumerate(((ahead0, behind0), (ahead1, behind1))):
        out[place] = mm(ahead[...], full[0], NT) + mm(behind[...], full[1], NN)


def near_terms_kernel(where, *refs):
    pieces = refs[: X * C]
    total, partner_near, diagonal_near, partner_far, diagonal_far, out, full = refs[X * C :]
    side = where[0]

    @pl.when(pl.program_id(0) == 0)
    def _():
        assemble(where, pieces, full)

    def add(partner_dims, diagonal_dims):
        for place, partner, diagonal in (
            (side, partner_near, diagonal_near),
            (1 - side, partner_far, diagonal_far),
        ):
            value = total[place] + mm(partner[...], full[0], partner_dims)
            value = value + mm(diagonal[...], full[1], diagonal_dims)
            out[place] = value.astype(out.dtype)

    @pl.when(side == 0)
    def _():
        add(NN, NT)

    @pl.when(side == 1)
    def _():
        add(NT, NN)


def term_call(kernel, where, pieces, total, blocks, dtype, name):
    half, n = blocks[0].shape
    rows = 256
    both = pl.BlockSpec((2, rows, n), lambda k, s: (0, k, 0))
    piece = pl.BlockSpec(pieces[0].shape, lambda k, s: (0, 0, 0))
    block = pl.BlockSpec((rows, n), lambda k, s: (k, 0))
    totals = [] if total is None else [total]
    return pl.pallas_call(
        kernel,
        grid_spec=pltpu.PrefetchScalarGridSpec(
            num_scalar_prefetch=1,
            grid=(half // rows,),
            in_specs=[piece] * len(pieces) + [both] * len(totals) + [block] * len(blocks),
            out_specs=both,
            scratch_shapes=[pltpu.VMEM((2, n, n), BF16)],
        ),
        out_shape=jax.ShapeDtypeStruct((2, half, n), dtype),
        name=name,
        cost_estimate=pl.CostEstimate(
            flops=8 * half * n * n, bytes_accessed=20 * half * n, transcendentals=0
        ),
    )(where, *pieces, *totals, *blocks)


def summed_rows(send, keep):
    paired = (keep + lax.ppermute(send, "c", [(0, 1), (1, 0)])).astype(BF16)
    blocks = lax.all_to_all(paired, "x", 0, 0, tiled=True)
    return jnp.sum(blocks.astype(F32), axis=0)


def amplitude_rows(sums, left_levels, right_levels):
    denominator = left_levels[:, None] + right_levels[None, :]
    return (SPIN_SCALE * sums / denominator).astype(BF16)


def gathered(rows):
    turns = [rows, moved(rows, "x", -1), moved(rows, "x", 2), moved(rows, "x", 1)]
    return turns + [lax.ppermute(t, "c", [(0, 1), (1, 0)]) for t in turns]


def on_device(three_index, occupied_energy, virtual_energy):
    rows, _, n = three_index.shape
    half = rows // 2
    own = three_index.reshape(rows, n)
    h, c, x = lax.axis_index("h"), lax.axis_index("c"), lax.axis_index("x")
    where = jnp.stack([h, c, x]).astype(jnp.int32)
    zh = lax.axis_size("z") * 2
    swap_h = [(0, 1), (1, 0)]
    along = [(i, (i + (2 if i % 2 == 0 else -2)) % zh) for i in range(zh)]
    across = [(i, (i + (1 if i % 2 else -1)) % zh) for i in range(zh)]

    low, high = own[:half], own[half:]
    near = lax.dynamic_slice_in_dim(own, h * half, half, 0)
    far = lax.dynamic_slice_in_dim(own, (1 - h) * half, half, 0)

    ahead1 = moved(high, "z", 1)
    behind0 = moved(low, "z", -1)
    partner_near = lax.ppermute(far, "h", swap_h)

    own_e = occupied_energy.astype(F32)
    ahead_e = moved(occupied_energy, "z", 1).astype(F32)
    behind_e = moved(occupied_energy, "z", -1).astype(F32)
    partner_e = lax.ppermute(occupied_energy, "h", swap_h).astype(F32)
    diagonal_e = lax.ppermute(occupied_energy, ("z", "h"), across).astype(F32)

    low2, high2, near2 = (after(v, ahead1, behind0, partner_near) for v in (low, high, near))
    ahead0 = moved(low2, "z", 1)
    behind1 = moved(high2, "z", -1)
    partner_far = lax.ppermute(near2, "h", swap_h)

    blocks = half // 256
    far_send, far_keep = pair_call(
        far_pairs_kernel,
        where,
        (own, ahead1, behind0, own),
        (
            lambda k, s: (blocks + k, 0),
            lambda k, s: (k, 0),
            lambda k, s: (k, 0),
            lambda k, s: (k, 0),
        ),
        half,
        n,
        "far_pairs",
    )
    near_send, near_keep = pair_call(
        near_pairs_kernel,
        where,
        (own, partner_near, ahead1, behind0),
        (
            lambda k, s: (s[0] * blocks + k, 0),
            lambda k, s: (k, 0),
            lambda k, s: (k, 0),
            lambda k, s: (k, 0),
        ),
        half,
        n,
        "near_pairs",
    )

    far_sums = summed_rows(far_send, far_keep)
    near_sums = summed_rows(near_send, near_keep)

    from_ahead = moved(far_sums[1].astype(BF16), "z", 1)
    from_behind = moved(far_sums[0].astype(BF16), "z", -1)
    near_wire = near_sums.astype(BF16)
    from_partner = lax.ppermute(near_wire, "h", swap_h)
    from_along = lax.ppermute(near_wire[1], ("z", "h"), along)

    share = n // (X * C)
    my_levels = lax.dynamic_slice_in_dim(virtual_energy, c * (n // C) + x * share, share, 0)
    even = h == 0

    def levels(left_e, right_e):
        return my_levels - left_e, virtual_energy - right_e

    far_rows = jnp.stack(
        [
            amplitude_rows(far_sums[0] + from_ahead.astype(F32), *levels(own_e, ahead_e)),
            amplitude_rows(far_sums[1] + from_behind.astype(F32), *levels(behind_e, own_e)),
        ]
    )
    near_rows = jnp.stack(
        [
            amplitude_rows(
                near_sums[0] + from_partner[0].astype(F32),
                *levels(jnp.where(even, partner_e, own_e), jnp.where(even, own_e, partner_e)),
            ),
            amplitude_rows(
                from_partner[1].astype(F32) + from_along.astype(F32),
                *levels(jnp.where(even, own_e, diagonal_e), jnp.where(even, diagonal_e, own_e)),
            ),
        ]
    )

    turned = jnp.where(even, behind0, ahead1)
    turned, along_near = (after(v, from_partner, from_along) for v in (turned, partner_near))
    diagonal_far = lax.ppermute(turned, "h", swap_h)
    diagonal_near = lax.ppermute(along_near, ("z", "h"), along)

    total = term_call(
        far_terms_kernel,
        where,
        gathered(far_rows),
        None,
        (ahead0, ahead1, behind0, behind1),
        F32,
        "far_terms",
    )
    density = term_call(
        near_terms_kernel,
        where,
        gathered(near_rows),
        total,
        (partner_near, diagonal_near, partner_far, diagonal_far),
        BF16,
        "near_terms",
    )
    return density.reshape(three_index.shape)


def solution(mesh):
    torus = Mesh(
        mesh.devices.reshape(mesh.shape["virt"], mesh.shape["occ"] // 2, 2, X, C),
        ("v", "z", "h", "x", "c"),
    )
    placed = P(("x", "c"), ("z", "h"), "v")
    return jax.shard_map(
        on_device,
        mesh=torus,
        in_specs=(placed, P(("z", "h")), P("v")),
        out_specs=placed,
        check_vma=False,
    )
```

```python
import jax
import jax.numpy as jnp
from jax import lax
from jax.experimental import pallas as pl
from jax.experimental.pallas import tpu as pltpu
from jax.sharding import Mesh
from jax.sharding import PartitionSpec as P


SPIN_SCALE = 1.2
X, C = 4, 2
F32, BF16 = jnp.float32, jnp.bfloat16
NN = (((1,), (0,)), ((), ()))
NT = (((1,), (1,)), ((), ()))


def mm(left, right, dims):
    return lax.dot_general(left, right, dims, preferred_element_type=F32)


def on_chip(kernel, where, operands, results, scratch, flops, off_chip=()):
    vmem, anywhere = (pl.BlockSpec(memory_space=m) for m in (pltpu.VMEM, pl.ANY))
    held = [pltpu.with_memory_space_constraint(v, pltpu.VMEM) for v in operands]
    chip = off_chip == ()
    return pl.pallas_call(
        kernel,
        in_specs=[pl.BlockSpec(memory_space=pltpu.SMEM)]
        + [anywhere] * len(off_chip or ())
        + [vmem] * len(held),
        out_specs=[vmem if chip else anywhere] * len(results),
        out_shape=[pltpu.VMEM(*r) if chip else jax.ShapeDtypeStruct(*r) for r in results],
        scratch_shapes=scratch,
        compiler_params=pltpu.CompilerParams(vmem_limit_bytes=20 << 20),
        cost_estimate=pl.CostEstimate(flops=flops, bytes_accessed=flops // 1000, transcendentals=0),
    )(where, *(off_chip or ()), *held)


def ring(axis, distance):
    size = lax.axis_size(axis)
    return [(i, (i + distance) % size) for i in range(size)]


def after(value, *events):
    return lax.optimization_barrier((value, *events))[0]


def add_products(core, lefts, rights, send, keep):
    part, n = send.shape[2:]
    half, strip = part * X, 256

    def step(j, carry):
        columns = pl.ds(pl.multiple_of(j * strip, strip), strip)
        for side, out in ((1 - core, send), (core, keep)):
            rows = pl.ds(pl.multiple_of(side * half, 128), half)
            for place in range(2):
                product = mm(lefts[place][rows, :], rights[place][:, columns], NN)
                for k in range(X):
                    out[k, place, :, columns] = product[k * part : (k + 1) * part]
        return carry

    lax.fori_loop(0, n // strip, step, 0)


def turn(block, out):
    strip = 256

    def step(j, carry):
        part = pl.ds(pl.multiple_of(j * strip, strip), strip)
        out[part, :] = block[:, part].T
        return carry

    lax.fori_loop(0, block.shape[1] // strip, step, 0)


def far_pairs_kernel(where, own_high, behind, ahead, own_low, send, keep, *lefts):
    turn(own_high, lefts[0])
    turn(behind, lefts[1])
    add_products(where[1], lefts, (ahead, own_low), send, keep)


def near_pairs_kernel(where, behind, partner, ahead, own, send, keep, *lefts):
    @pl.when(where[0] == 0)
    def _():
        turn(partner, lefts[0])
        turn(behind, lefts[1])
        add_products(where[1], lefts, (own, partner), send, keep)

    @pl.when(where[0] == 1)
    def _():
        turn(own, lefts[0])
        turn(partner, lefts[1])
        add_products(where[1], lefts, (partner, ahead), send, keep)


def pair_call(kernel, where, operands):
    half, n = operands[-1].shape
    result = ((X, 2, n // (X * C), n), F32)
    lefts = [pltpu.VMEM((n, half), BF16)] * 2
    return on_chip(kernel, where, operands, [result, result], lefts, 4 * half * n * n)


def assemble(where, mine, other, full):
    part = mine.shape[2]
    core = where[1]
    for pieces, side in ((mine, core), (other, 1 - core)):
        for j in range(X):
            row = pl.multiple_of(side * (part * X) + j * part, 32)
            for place in range(2):
                full[place, pl.ds(row, part), :] = pieces[j, place]


STEP_ROWS = 256


def row_block(k):
    return pl.ds(pl.multiple_of(k * STEP_ROWS, STEP_ROWS), STEP_ROWS)


def far_terms_kernel(
    where, mine, other, ahead0, ahead1, behind0, behind1, out, full, ready, sent
):
    assemble(where, mine, other, full)
    steps = ahead0.shape[0] // STEP_ROWS

    def sending(k):
        rows = row_block(k)
        return pltpu.make_async_copy(ready.at[:, rows, :], out.at[:, rows, :], sent.at[k])

    def step(k, carry):
        rows = row_block(k)
        for place, (ahead, behind) in enumerate(((ahead0, behind0), (ahead1, behind1))):
            value = mm(ahead[rows, :], full[0], NT) + mm(behind[rows, :], full[1], NN)
            ready[place, rows, :] = value
        sending(k).start()
        return carry

    lax.fori_loop(0, steps, step, 0)
    for k in range(steps):
        sending(k).wait()


def near_terms_kernel(where, total, mine, other, *refs):
    partner_near, partner_far, near_a, near_b, far_a, far_b = refs[:6]
    out, full, loaded, ready, arrived, sent = refs[6:]
    steps = near_a.shape[0] // STEP_ROWS

    def loading(k):
        rows = row_block(k)
        return pltpu.make_async_copy(total.at[:, rows, :], loaded.at[:, rows, :], arrived.at[k])

    def sending(k):
        rows = row_block(k)
        return pltpu.make_async_copy(ready.at[:, rows, :], out.at[:, rows, :], sent.at[k])

    for k in range(2 * steps):
        loading(k).start()
    assemble(where, mine, other, full)

    def add(side, partner_dims, diagonal_dims):
        for part, diagonals in enumerate(((near_a, far_a), (near_b, far_b))):

            def step(k, carry, part=part, diagonals=diagonals):
                local, number = row_block(k), part * steps + k
                rows = row_block(number)
                loading(number).wait()
                for place, partner, diagonal in (
                    (side, partner_near, diagonals[0]),
                    (1 - side, partner_far, diagonals[1]),
                ):
                    value = loaded[place, rows, :] + mm(partner[rows, :], full[0], partner_dims)
                    value = value + mm(diagonal[local, :], full[1], diagonal_dims)
                    ready[place, rows, :] = value.astype(ready.dtype)
                sending(number).start()
                return carry

            lax.fori_loop(0, steps, step, 0)

    @pl.when(where[0] == 0)
    def _():
        add(0, NN, NT)

    @pl.when(where[0] == 1)
    def _():
        add(1, NT, NN)

    for k in range(2 * steps):
        sending(k).wait()


def core_swap(value):
    return lax.ppermute(value, "c", [(0, 1), (1, 0)])


def exchanged(blocks):
    return lax.all_to_all(blocks, "x", 0, 0, tiled=True)


def summed_rows(send, keep):
    paired = (keep + core_swap(send)).astype(BF16)
    return jnp.sum(exchanged(paired).astype(F32), axis=0)


def amplitude_rows(sums, left_levels, right_levels):
    denominator = left_levels[:, None] + right_levels[None, :]
    return (SPIN_SCALE * sums / denominator).astype(BF16)


def gathered(rows):
    mine = exchanged(jnp.broadcast_to(rows, (X, *rows.shape)))
    return mine, core_swap(mine)


def on_device(three_index, occupied_energy, virtual_energy):
    rows, _, n = three_index.shape
    half, quarter = rows // 2, rows // 4
    own = three_index.reshape(rows, n)
    h, c, x = lax.axis_index("h"), lax.axis_index("c"), lax.axis_index("x")
    where = jnp.stack([h, c, x]).astype(jnp.int32)
    even = h == 0
    zh = lax.axis_size("z") * 2
    swap_h = [(0, 1), (1, 0)]
    along_route = [(i, (i + (2 if i % 2 == 0 else -2)) % zh) for i in range(zh)]

    def ahead_of(value):
        return lax.ppermute(value, "z", ring("z", 1))

    def behind_of(value):
        return lax.ppermute(value, "z", ring("z", -1))

    def partner_of(value):
        return lax.ppermute(value, "h", swap_h)

    def along(value):
        return lax.ppermute(value, ("z", "h"), along_route)

    def energy(axis, route):
        return lax.ppermute(occupied_energy, axis, route).astype(F32)

    def cut(value, start, length):
        return lax.dynamic_slice_in_dim(value, start, length, 0)

    high = cut(own, half, half)
    low = cut(after(own, high), 0, half)
    far = cut(after(own, low), (1 - h) * half, half)
    near = cut(after(own, far), h * half, half)
    ahead1 = ahead_of(high)
    behind0 = behind_of(low)
    partner_near = partner_of(far)

    ahead0 = ahead_of(low)
    behind1 = behind_of(high)
    partner_far = partner_of(near)

    own_e = occupied_energy.astype(F32)
    ahead_e = energy("z", ring("z", 1))
    behind_e = energy("z", ring("z", -1))
    partner_e = energy("h", swap_h)
    diagonal_e = energy(("z", "h"), [(i, (i + (1 if i % 2 else -1)) % zh) for i in range(zh)])

    far_send, far_keep = pair_call(far_pairs_kernel, where, (high, behind0, ahead1, low))
    near_send, near_keep = pair_call(
        near_pairs_kernel, where, (behind0, partner_near, ahead1, near)
    )

    def facing(start):
        cuts = (v[start : start + quarter] for v in (behind0, ahead1))
        return jnp.where(even, *cuts)

    far_a = partner_of(facing(0))
    far_b = partner_of(facing(quarter))
    near_a = along(partner_near[:quarter])
    near_b = along(partner_near[quarter:])

    far_sums = summed_rows(far_send, far_keep)
    near_sums = summed_rows(near_send, near_keep)

    far_wire = far_sums.astype(BF16)
    from_ahead = ahead_of(far_wire[1])
    from_behind = behind_of(far_wire[0])
    near_wire = near_sums.astype(BF16)
    from_partner = partner_of(near_wire)
    from_along = along(near_wire[1])

    share = n // (X * C)
    my_levels = lax.dynamic_slice_in_dim(virtual_energy, c * (n // C) + x * share, share, 0)

    def levels(left_e, right_e):
        return my_levels - left_e, virtual_energy - right_e

    far_rows = jnp.stack(
        [
            amplitude_rows(far_sums[0] + from_ahead.astype(F32), *levels(own_e, ahead_e)),
            amplitude_rows(far_sums[1] + from_behind.astype(F32), *levels(behind_e, own_e)),
        ]
    )
    from_partner = after(from_partner, far_rows)
    near_rows = jnp.stack(
        [
            amplitude_rows(
                near_sums[0] + from_partner[0].astype(F32),
                *levels(jnp.where(even, partner_e, own_e), jnp.where(even, own_e, partner_e)),
            ),
            amplitude_rows(
                from_partner[1].astype(F32) + from_along.astype(F32),
                *levels(jnp.where(even, own_e, diagonal_e), jnp.where(even, diagonal_e, own_e)),
            ),
        ]
    )

    full = pltpu.VMEM((2, n, n), BF16)
    copies = pltpu.SemaphoreType.DMA((half // STEP_ROWS,))
    work = 8 * half * n * n
    (total,) = on_chip(
        far_terms_kernel,
        where,
        (*gathered(far_rows), ahead0, ahead1, behind0, behind1),
        [((2, half, n), F32)],
        [full, pltpu.VMEM((2, half, n), F32), copies],
        work,
        off_chip=None,
    )
    (density,) = on_chip(
        near_terms_kernel,
        where,
        (
            *gathered(near_rows),
            *(partner_near, partner_far, near_a, near_b, far_a, far_b),
        ),
        [((2, half, n), BF16)],
        [
            full,
            pltpu.VMEM((2, half, n), F32),
            pltpu.VMEM((2, half, n), BF16),
            copies,
            copies,
        ],
        work,
        off_chip=(total,),
    )
    return density.reshape(three_index.shape)


def solution(mesh):
    torus = Mesh(
        mesh.devices.reshape(mesh.shape["virt"], mesh.shape["occ"] // 2, 2, X, C),
        ("v", "z", "h", "x", "c"),
    )
    placed = P(("x", "c"), ("z", "h"), "v")
    return jax.shard_map(
        on_device,
        mesh=torus,
        in_specs=(placed, P(("z", "h")), P("v")),
        out_specs=placed,
        check_vma=False,
    )
```

```python
import jax
import jax.numpy as jnp
from jax import lax
from jax.experimental import pallas as pl
from jax.experimental.pallas import tpu as pltpu
from jax.sharding import Mesh
from jax.sharding import PartitionSpec as P


SPIN_SCALE = 1.2
X, C = 4, 2
F32, BF16 = jnp.float32, jnp.bfloat16
NN = (((1,), (0,)), ((), ()))
NT = (((1,), (1,)), ((), ()))


def mm(left, right, dims):
    return lax.dot_general(left, right, dims, preferred_element_type=F32)


def on_chip(kernel, where, operands, results, scratch, flops, off_chip=()):
    vmem, hbm = (pl.BlockSpec(memory_space=m) for m in (pltpu.VMEM, pltpu.HBM))
    held = [pltpu.with_memory_space_constraint(v, pltpu.VMEM) for v in operands]
    far_away = [pltpu.with_memory_space_constraint(v, pltpu.HBM) for v in off_chip]
    return pl.pallas_call(
        kernel,
        in_specs=[pl.BlockSpec(memory_space=pltpu.SMEM)]
        + [hbm] * len(far_away)
        + [vmem] * len(held),
        out_specs=[hbm] * len(results),
        out_shape=[pltpu.HBM(*r) for r in results],
        scratch_shapes=scratch,
        compiler_params=pltpu.CompilerParams(vmem_limit_bytes=20 << 20),
        cost_estimate=pl.CostEstimate(flops=flops, bytes_accessed=flops // 1000, transcendentals=0),
    )(where, *far_away, *held)


def ring(axis, distance):
    size = lax.axis_size(axis)
    return [(i, (i + distance) % size) for i in range(size)]


def moved(value, axis, distance):
    return lax.ppermute(value, axis, ring(axis, distance))


def after(value, *events):
    return lax.optimization_barrier((value, *events))[0]


STRIP = 256


def add_products(core, first, lefts, rights, outs, ready, sent):
    part, n = ready.shape[3:]
    half = part * X

    def sending(j, number):
        columns = pl.ds(pl.multiple_of(j * STRIP, STRIP), STRIP)
        source = ready.at[number, :, :, :, columns]
        return pltpu.make_async_copy(source, outs[number].at[:, :, :, columns], sent.at[j, number])

    def step(j, carry):
        columns = pl.ds(pl.multiple_of(j * STRIP, STRIP), STRIP)
        for number, side in enumerate((1 - core, core)):
            rows = pl.ds(pl.multiple_of(side * half, 128), half)
            for place in range(2):
                product = mm(lefts[place][rows, :], rights[place][:, columns], NN)
                for k in range(X):
                    chunk = lax.rem(k - first + X, X)
                    ready[number, chunk, place, :, columns] = product[k * part : (k + 1) * part]
            sending(j, number).start()
        return carry

    lax.fori_loop(0, n // STRIP, step, 0)
    for j in range(n // STRIP):
        for number in range(2):
            sending(j, number).wait()


def turn(block, out):
    strip = 256

    def step(j, carry):
        part = pl.ds(pl.multiple_of(j * strip, strip), strip)
        out[part, :] = block[:, part].T
        return carry

    lax.fori_loop(0, block.shape[1] // strip, step, 0)


def far_pairs_kernel(where, own_high, behind, ahead, own_low, *refs):
    outs, lefts, (ready, sent) = refs[:2], refs[2:4], refs[4:]
    turn(own_high, lefts[0])
    turn(behind, lefts[1])
    add_products(where[1], 0, lefts, (ahead, own_low), outs, ready, sent)


def near_pairs_kernel(where, behind, partner, ahead, own, *refs):
    outs, lefts, (ready, sent) = refs[:2], refs[2:4], refs[4:]
    core, x = where[1], where[2]

    @pl.when(where[0] == 0)
    def _():
        turn(partner, lefts[0])
        turn(behind, lefts[1])
        add_products(core, x, lefts, (own, partner), outs, ready, sent)

    @pl.when(where[0] == 1)
    def _():
        turn(own, lefts[0])
        turn(partner, lefts[1])
        add_products(core, x, lefts, (partner, ahead), outs, ready, sent)


def pair_call(kernel, where, operands):
    half, n = operands[-1].shape
    shape = (X, 2, n // (X * C), n)
    scratch = [pltpu.VMEM((n, half), BF16)] * 2
    scratch += [pltpu.VMEM((2, *shape), F32), pltpu.SemaphoreType.DMA((n // STRIP, 2))]
    return on_chip(kernel, where, operands, [(shape, F32)] * 2, scratch, 4 * half * n * n)


def assemble(where, mine, other, full):
    part = mine.shape[2]
    core = where[1]
    for pieces, side in ((mine, core), (other, 1 - core)):
        for j in range(X):
            row = pl.multiple_of(side * (part * X) + j * part, 32)
            for place in range(2):
                full[place, pl.ds(row, part), :] = pieces[j, place]


STEP_ROWS = 256


def row_block(k):
    return pl.ds(pl.multiple_of(k * STEP_ROWS, STEP_ROWS), STEP_ROWS)


def far_terms_kernel(
    where, mine, other, ahead0, ahead1, behind0, behind1, out, full, ready, sent
):
    assemble(where, mine, other, full)
    steps = ahead0.shape[0] // STEP_ROWS

    def sending(k):
        rows = row_block(k)
        return pltpu.make_async_copy(ready.at[:, rows, :], out.at[:, rows, :], sent.at[k])

    def step(k, carry):
        rows = row_block(k)
        for place, (ahead, behind) in enumerate(((ahead0, behind0), (ahead1, behind1))):
            value = mm(ahead[rows, :], full[0], NT) + mm(behind[rows, :], full[1], NN)
            ready[place, rows, :] = value
        sending(k).start()
        return carry

    lax.fori_loop(0, steps, step, 0)
    for k in range(steps):
        sending(k).wait()


def assemble_turned(where, pieces, full):
    part = pieces[0].shape[1]
    core, x = where[1], where[2]
    for number, piece in enumerate(pieces):
        turn_by, other = number % X, number // X
        row = lax.rem(core + other, C) * (part * X) + lax.rem(x - turn_by + X, X) * part
        for place in range(2):
            full[place, pl.ds(pl.multiple_of(row, 32), part), :] = piece[place]


def near_terms_kernel(where, total, *refs):
    pieces, refs = refs[: X * C], refs[X * C :]
    partner_near, partner_far, near_a, near_b, far_a, far_b = refs[:6]
    out, full, loaded, ready, arrived, sent = refs[6:]
    steps = near_a.shape[0] // STEP_ROWS

    def loading(k):
        rows = row_block(k)
        return pltpu.make_async_copy(total.at[:, rows, :], loaded.at[:, rows, :], arrived.at[k])

    def sending(k):
        rows = row_block(k)
        return pltpu.make_async_copy(ready.at[:, rows, :], out.at[:, rows, :], sent.at[k])

    for k in range(2 * steps):
        loading(k).start()
    assemble_turned(where, pieces, full)

    def add(side, partner_dims, diagonal_dims):
        for part, diagonals in enumerate(((near_a, far_a), (near_b, far_b))):

            def step(k, carry, part=part, diagonals=diagonals):
                local, number = row_block(k), part * steps + k
                rows = row_block(number)
                loading(number).wait()
                for place, partner, diagonal in (
                    (side, partner_near, diagonals[0]),
                    (1 - side, partner_far, diagonals[1]),
                ):
                    value = loaded[place, rows, :] + mm(partner[rows, :], full[0], partner_dims)
                    value = value + mm(diagonal[local, :], full[1], diagonal_dims)
                    ready[place, rows, :] = value.astype(ready.dtype)
                sending(number).start()
                return carry

            lax.fori_loop(0, steps, step, 0)

    @pl.when(where[0] == 0)
    def _():
        add(0, NN, NT)

    @pl.when(where[0] == 1)
    def _():
        add(1, NT, NN)

    for k in range(2 * steps):
        sending(k).wait()


def core_swap(value):
    return lax.ppermute(value, "c", [(0, 1), (1, 0)])


def exchanged(blocks):
    return lax.all_to_all(blocks, "x", 0, 0, tiled=True)


def summed_rows(paired):
    return jnp.sum(exchanged(paired).astype(F32), axis=0)


def turned_in(values):
    results = []
    for t, value in enumerate(values):
        results.append(moved(value, "x", t + 1))
    return results


def turned_sum(send, keep):
    other = core_swap(send)
    mine, *rest = (keep[t] + other[t] for t in range(X))
    for piece in turned_in([r.astype(BF16) for r in rest]):
        mine = mine + piece.astype(F32)
    return mine


def turned_gather(rows):
    pieces = [rows, *turned_in([rows] * (X - 1))]
    return pieces + [core_swap(p) for p in pieces]


def amplitude_rows(sums, left_levels, right_levels):
    denominator = left_levels[:, None] + right_levels[None, :]
    return (SPIN_SCALE * sums / denominator).astype(BF16)


def gathered(rows):
    mine = exchanged(jnp.broadcast_to(rows, (X, *rows.shape)))
    return mine, core_swap(mine)


def on_device(three_index, occupied_energy, virtual_energy):
    rows, _, n = three_index.shape
    half, quarter = rows // 2, rows // 4
    own = three_index.reshape(rows, n)
    h, c, x = lax.axis_index("h"), lax.axis_index("c"), lax.axis_index("x")
    where = jnp.stack([h, c, x]).astype(jnp.int32)
    even = h == 0
    zh = lax.axis_size("z") * 2
    swap_h = [(0, 1), (1, 0)]
    along_route = [(i, (i + (2 if i % 2 == 0 else -2)) % zh) for i in range(zh)]

    def ahead_of(value):
        return lax.ppermute(value, "z", ring("z", 1))

    def behind_of(value):
        return lax.ppermute(value, "z", ring("z", -1))

    def partner_of(value):
        return lax.ppermute(value, "h", swap_h)

    def along(value):
        return lax.ppermute(value, ("z", "h"), along_route)

    def energy(axis, route):
        return lax.ppermute(occupied_energy, axis, route)

    def cut(value, start, length):
        return lax.dynamic_slice_in_dim(value, start, length, 0)

    high = cut(own, half, half)
    low = cut(after(own, high), 0, half)
    far = cut(after(own, low), (1 - h) * half, half)
    near = cut(after(own, far), h * half, half)
    ahead1 = ahead_of(high)
    behind0 = behind_of(low)
    partner_near = partner_of(far)

    ahead0 = ahead_of(low)
    behind1 = behind_of(high)
    partner_far = partner_of(near)

    own_e = occupied_energy.astype(F32)
    ahead_e = energy("z", ring("z", 1))
    behind_e = energy("z", ring("z", -1))
    partner_e = energy("h", swap_h)
    diagonal_e = energy(("z", "h"), [(i, (i + (1 if i % 2 else -1)) % zh) for i in range(zh)])

    far_send, far_keep = pair_call(far_pairs_kernel, where, (high, behind0, ahead1, low))
    near_send, near_keep = pair_call(
        near_pairs_kernel, where, (behind0, partner_near, ahead1, near)
    )

    def facing(start):
        cuts = (v[start : start + quarter] for v in (behind0, ahead1))
        return jnp.where(even, *cuts)

    far_a = partner_of(facing(0))
    far_b = partner_of(facing(quarter))
    near_a = along(partner_near[:quarter])
    near_b = along(partner_near[quarter:])

    paired = (far_keep + core_swap(far_send)).astype(BF16)
    far_sums = summed_rows(paired)
    near_sums = turned_sum(near_send, near_keep)
    ahead_e, behind_e, partner_e, diagonal_e = (
        after(e, paired).astype(F32) for e in (ahead_e, behind_e, partner_e, diagonal_e)
    )

    far_wire = far_sums.astype(BF16)
    from_ahead = ahead_of(far_wire[1])
    from_behind = behind_of(far_wire[0])
    near_wire = near_sums.astype(BF16)
    from_partner = partner_of(near_wire)
    from_along = along(near_wire[1])

    share = n // (X * C)
    my_levels = lax.dynamic_slice_in_dim(virtual_energy, c * (n // C) + x * share, share, 0)

    def levels(left_e, right_e):
        return my_levels - left_e, virtual_energy - right_e

    far_rows = jnp.stack(
        [
            amplitude_rows(far_sums[0] + from_ahead.astype(F32), *levels(own_e, ahead_e)),
            amplitude_rows(far_sums[1] + from_behind.astype(F32), *levels(behind_e, own_e)),
        ]
    )
    from_partner = after(from_partner, far_rows)
    near_rows = jnp.stack(
        [
            amplitude_rows(
                near_sums[0] + from_partner[0].astype(F32),
                *levels(jnp.where(even, partner_e, own_e), jnp.where(even, own_e, partner_e)),
            ),
            amplitude_rows(
                from_partner[1].astype(F32) + from_along.astype(F32),
                *levels(jnp.where(even, own_e, diagonal_e), jnp.where(even, diagonal_e, own_e)),
            ),
        ]
    )

    full = pltpu.VMEM((2, n, n), BF16)
    copies = pltpu.SemaphoreType.DMA((half // STEP_ROWS,))
    work = 8 * half * n * n
    (total,) = on_chip(
        far_terms_kernel,
        where,
        (*gathered(far_rows), ahead0, ahead1, behind0, behind1),
        [((2, half, n), F32)],
        [full, pltpu.VMEM((2, half, n), F32), copies],
        work,
    )
    (density,) = on_chip(
        near_terms_kernel,
        where,
        (
            *turned_gather(near_rows),
            *(partner_near, partner_far, near_a, near_b, far_a, far_b),
        ),
        [((2, half, n), BF16)],
        [
            full,
            pltpu.VMEM((2, half, n), F32),
            pltpu.VMEM((2, half, n), BF16),
            copies,
            copies,
        ],
        work,
        off_chip=(total,),
    )
    return density.reshape(three_index.shape)


def solution(mesh):
    torus = Mesh(
        mesh.devices.reshape(mesh.shape["virt"], mesh.shape["occ"] // 2, 2, X, C),
        ("v", "z", "h", "x", "c"),
    )
    placed = P(("x", "c"), ("z", "h"), "v")
    return jax.shard_map(
        on_device,
        mesh=torus,
        in_specs=(placed, P(("z", "h")), P("v")),
        out_specs=placed,
        check_vma=False,
    )
```

```python
import jax
import jax.numpy as jnp
from jax import lax
from jax.experimental import pallas as pl
from jax.experimental.pallas import tpu as pltpu
from jax.sharding import Mesh
from jax.sharding import PartitionSpec as P


SPIN_SCALE = 1.2
X, C = 4, 2
F32, BF16 = jnp.float32, jnp.bfloat16
NN = (((1,), (0,)), ((), ()))
NT = (((1,), (1,)), ((), ()))


def mm(left, right, dims):
    return lax.dot_general(left, right, dims, preferred_element_type=F32)


def on_chip(kernel, where, operands, results, scratch, flops, off_chip=()):
    vmem, hbm = (pl.BlockSpec(memory_space=m) for m in (pltpu.VMEM, pltpu.HBM))
    held = [pltpu.with_memory_space_constraint(v, pltpu.VMEM) for v in operands]
    far_away = [pltpu.with_memory_space_constraint(v, pltpu.HBM) for v in off_chip]
    return pl.pallas_call(
        kernel,
        in_specs=[pl.BlockSpec(memory_space=pltpu.SMEM)]
        + [hbm] * len(far_away)
        + [vmem] * len(held),
        out_specs=[hbm] * len(results),
        out_shape=[pltpu.HBM(*r) for r in results],
        scratch_shapes=scratch,
        compiler_params=pltpu.CompilerParams(vmem_limit_bytes=20 << 20),
        cost_estimate=pl.CostEstimate(flops=flops, bytes_accessed=flops // 1000, transcendentals=0),
    )(where, *far_away, *held)


def ring(axis, distance):
    size = lax.axis_size(axis)
    return [(i, (i + distance) % size) for i in range(size)]


def moved(value, axis, distance):
    return lax.ppermute(value, axis, ring(axis, distance))


def after(value, *events):
    return lax.optimization_barrier((value, *events))[0]


STRIP = 256


def add_products(core, first, lefts, rights, outs, ready, sent):
    part, n = ready.shape[3:]
    half = part * X

    def sending(j, number):
        columns = pl.ds(pl.multiple_of(j * STRIP, STRIP), STRIP)
        source = ready.at[number, :, :, :, columns]
        return pltpu.make_async_copy(source, outs[number].at[:, :, :, columns], sent.at[j, number])

    def step(j, carry):
        columns = pl.ds(pl.multiple_of(j * STRIP, STRIP), STRIP)
        for number, side in enumerate((1 - core, core)):
            rows = pl.ds(pl.multiple_of(side * half, 128), half)
            for place in range(2):
                product = mm(lefts[place][rows, :], rights[place][:, columns], NN)
                for k in range(X):
                    chunk = lax.rem(k - first + X, X)
                    ready[number, chunk, place, :, columns] = product[k * part : (k + 1) * part]
            sending(j, number).start()
        return carry

    lax.fori_loop(0, n // STRIP, step, 0)
    for j in range(n // STRIP):
        for number in range(2):
            sending(j, number).wait()


def turn(block, out):
    strip = 256

    def step(j, carry):
        part = pl.ds(pl.multiple_of(j * strip, strip), strip)
        out[part, :] = block[:, part].T
        return carry

    lax.fori_loop(0, block.shape[1] // strip, step, 0)


def far_pairs_kernel(where, own_high, behind, ahead, own_low, *refs):
    outs, lefts, (ready, sent) = refs[:2], refs[2:4], refs[4:]
    turn(own_high, lefts[0])
    turn(behind, lefts[1])
    add_products(where[1], 0, lefts, (ahead, own_low), outs, ready, sent)


def near_pairs_kernel(where, behind, partner, ahead, own, *refs):
    outs, lefts, (ready, sent) = refs[:2], refs[2:4], refs[4:]
    core, x = where[1], where[2]

    @pl.when(where[0] == 0)
    def _():
        turn(partner, lefts[0])
        turn(behind, lefts[1])
        add_products(core, x, lefts, (own, partner), outs, ready, sent)

    @pl.when(where[0] == 1)
    def _():
        turn(own, lefts[0])
        turn(partner, lefts[1])
        add_products(core, x, lefts, (partner, ahead), outs, ready, sent)


def copy_kernel(value, out):
    for k in range(value.shape[0]):
        out[k] = value[k]


def copied(value):
    table = pl.BlockSpec(memory_space=pltpu.SMEM)
    return pl.pallas_call(
        copy_kernel,
        in_specs=[table],
        out_specs=table,
        out_shape=jax.ShapeDtypeStruct(value.shape, value.dtype),
    )(value)


def pair_call(kernel, where, operands):
    half, n = operands[-1].shape
    shape = (X, 2, n // (X * C), n)
    scratch = [pltpu.VMEM((n, half), BF16)] * 2
    scratch += [pltpu.VMEM((2, *shape), F32), pltpu.SemaphoreType.DMA((n // STRIP, 2))]
    return on_chip(kernel, where, operands, [(shape, F32)] * 2, scratch, 4 * half * n * n)


def assemble(where, mine, other, full):
    part = mine.shape[2]
    core = where[1]
    for pieces, side in ((mine, core), (other, 1 - core)):
        for j in range(X):
            row = pl.multiple_of(side * (part * X) + j * part, 32)
            for place in range(2):
                full[place, pl.ds(row, part), :] = pieces[j, place]


STEP_ROWS = 256


def row_block(k):
    return pl.ds(pl.multiple_of(k * STEP_ROWS, STEP_ROWS), STEP_ROWS)


def far_terms_kernel(
    where, mine, other, ahead0, ahead1, behind0, behind1, out, full, ready, sent
):
    assemble(where, mine, other, full)
    steps = ahead0.shape[0] // STEP_ROWS

    def sending(k):
        rows = row_block(k)
        return pltpu.make_async_copy(ready.at[:, rows, :], out.at[:, rows, :], sent.at[k])

    def step(k, carry):
        rows = row_block(k)
        for place, (ahead, behind) in enumerate(((ahead0, behind0), (ahead1, behind1))):
            value = mm(ahead[rows, :], full[0], NT) + mm(behind[rows, :], full[1], NN)
            ready[place, rows, :] = value
        sending(k).start()
        return carry

    lax.fori_loop(0, steps, step, 0)
    for k in range(steps):
        sending(k).wait()


def assemble_turned(where, pieces, full):
    part = pieces[0].shape[1]
    core, x = where[1], where[2]
    for number, piece in enumerate(pieces):
        turn_by, other = number % X, number // X
        row = lax.rem(core + other, C) * (part * X) + lax.rem(x - turn_by + X, X) * part
        for place in range(2):
            full[place, pl.ds(pl.multiple_of(row, 32), part), :] = piece[place]


def near_terms_kernel(where, total, *refs):
    pieces, refs = refs[: X * C], refs[X * C :]
    partner_near, partner_far, near_a, near_b, far_a, far_b = refs[:6]
    out, full, loaded, ready, arrived, sent = refs[6:]
    steps = near_a.shape[0] // STEP_ROWS

    def loading(k):
        rows = row_block(k)
        return pltpu.make_async_copy(total.at[:, rows, :], loaded.at[:, rows, :], arrived.at[k])

    def sending(k):
        rows = row_block(k)
        return pltpu.make_async_copy(ready.at[:, rows, :], out.at[:, rows, :], sent.at[k])

    for k in range(2 * steps):
        loading(k).start()
    assemble_turned(where, pieces, full)

    def add(side, partner_dims, diagonal_dims):
        for part, diagonals in enumerate(((near_a, far_a), (near_b, far_b))):

            def step(k, carry, part=part, diagonals=diagonals):
                local, number = row_block(k), part * steps + k
                rows = row_block(number)
                loading(number).wait()
                for place, partner, diagonal in (
                    (side, partner_near, diagonals[0]),
                    (1 - side, partner_far, diagonals[1]),
                ):
                    value = loaded[place, rows, :] + mm(partner[rows, :], full[0], partner_dims)
                    value = value + mm(diagonal[local, :], full[1], diagonal_dims)
                    ready[place, rows, :] = value.astype(ready.dtype)
                sending(number).start()
                return carry

            lax.fori_loop(0, steps, step, 0)

    @pl.when(where[0] == 0)
    def _():
        add(0, NN, NT)

    @pl.when(where[0] == 1)
    def _():
        add(1, NT, NN)

    for k in range(2 * steps):
        sending(k).wait()


def core_swap(value):
    return lax.ppermute(value, "c", [(0, 1), (1, 0)])


def exchanged(blocks):
    return lax.all_to_all(blocks, "x", 0, 0, tiled=True)


def summed_rows(paired):
    return jnp.sum(exchanged(paired).astype(F32), axis=0)


def turned_in(values):
    results = []
    for t, value in enumerate(values):
        results.append(moved(value, "x", t + 1))
    return results


def turned_sum(send, keep):
    other = core_swap(send)
    mine, *rest = (keep[t] + other[t] for t in range(X))
    rest = [r.astype(BF16) for r in rest]
    pieces = turned_in(rest)
    for piece in pieces:
        mine = mine + piece.astype(F32)
    return mine


def turned_gather(rows):
    pieces = [rows, *turned_in([rows] * (X - 1))]
    return pieces + [core_swap(p) for p in pieces]


def amplitude_rows(sums, left_levels, right_levels):
    denominator = left_levels[:, None] + right_levels[None, :]
    return (SPIN_SCALE * sums / denominator).astype(BF16)


def gathered(rows):
    mine = exchanged(jnp.broadcast_to(rows, (X, *rows.shape)))
    return mine, core_swap(mine)


def on_device(three_index, occupied_energy, virtual_energy):
    rows, _, n = three_index.shape
    half, quarter = rows // 2, rows // 4
    own = three_index.reshape(rows, n)
    h, c, x = lax.axis_index("h"), lax.axis_index("c"), lax.axis_index("x")
    where = jnp.stack([h, c, x]).astype(jnp.int32)
    even = h == 0
    zh = lax.axis_size("z") * 2
    swap_h = [(0, 1), (1, 0)]
    along_route = [(i, (i + (2 if i % 2 == 0 else -2)) % zh) for i in range(zh)]

    def ahead_of(value):
        return lax.ppermute(value, "z", ring("z", 1))

    def behind_of(value):
        return lax.ppermute(value, "z", ring("z", -1))

    def partner_of(value):
        return lax.ppermute(value, "h", swap_h)

    def along(value):
        return lax.ppermute(value, ("z", "h"), along_route)

    def energy(axis, route):
        return lax.ppermute(occupied_energy, axis, route)

    def cut(value, start, length):
        return lax.dynamic_slice_in_dim(value, start, length, 0)

    high = cut(own, half, half)
    low = cut(after(own, high), 0, half)
    far = cut(after(own, low), (1 - h) * half, half)
    near = cut(after(own, far), h * half, half)
    ahead1 = ahead_of(high)
    behind0 = behind_of(low)
    partner_near = partner_of(far)

    ahead0 = ahead_of(low)
    behind1 = behind_of(high)
    partner_far = partner_of(near)

    own_e = occupied_energy.astype(F32)
    ahead_e = energy("z", ring("z", 1))
    behind_e = energy("z", ring("z", -1))
    partner_e = energy("h", swap_h)
    diagonal_e = energy(("z", "h"), [(i, (i + (1 if i % 2 else -1)) % zh) for i in range(zh)])

    far_send, far_keep = pair_call(far_pairs_kernel, where, (high, behind0, ahead1, low))
    near_send, near_keep = pair_call(
        near_pairs_kernel, where, (behind0, partner_near, ahead1, near)
    )

    def facing(start):
        cuts = (v[start : start + quarter] for v in (behind0, ahead1))
        return jnp.where(even, *cuts)

    far_a = partner_of(facing(0))
    far_b = partner_of(facing(quarter))
    near_a = along(partner_near[:quarter])
    near_b = along(partner_near[quarter:])

    paired = (far_keep + core_swap(far_send)).astype(BF16)
    far_sums = summed_rows(paired)
    near_sums = turned_sum(near_send, near_keep)
    ahead_e, behind_e, partner_e, diagonal_e = (
        after(e, paired).astype(F32) for e in (ahead_e, behind_e, partner_e, diagonal_e)
    )

    far_wire = far_sums.astype(BF16)
    from_ahead = ahead_of(far_wire[1])
    from_behind = behind_of(far_wire[0])
    near_wire = near_sums.astype(BF16)
    from_partner = partner_of(near_wire)
    from_along = along(near_wire[1])

    share = n // (X * C)
    my_levels = lax.dynamic_slice_in_dim(virtual_energy, c * (n // C) + x * share, share, 0)

    def levels(left_e, right_e):
        return my_levels - left_e, virtual_energy - right_e

    far_rows = jnp.stack(
        [
            amplitude_rows(far_sums[0] + from_ahead.astype(F32), *levels(own_e, ahead_e)),
            amplitude_rows(far_sums[1] + from_behind.astype(F32), *levels(behind_e, own_e)),
        ]
    )
    from_partner = after(from_partner, far_rows)
    near_rows = jnp.stack(
        [
            amplitude_rows(
                near_sums[0] + from_partner[0].astype(F32),
                *levels(jnp.where(even, partner_e, own_e), jnp.where(even, own_e, partner_e)),
            ),
            amplitude_rows(
                from_partner[1].astype(F32) + from_along.astype(F32),
                *levels(jnp.where(even, own_e, diagonal_e), jnp.where(even, diagonal_e, own_e)),
            ),
        ]
    )

    full = pltpu.VMEM((2, n, n), BF16)
    copies = pltpu.SemaphoreType.DMA((half // STEP_ROWS,))
    work = 8 * half * n * n
    (total,) = on_chip(
        far_terms_kernel,
        copied(where),
        (*gathered(far_rows), ahead0, ahead1, behind0, behind1),
        [((2, half, n), F32)],
        [full, pltpu.VMEM((2, half, n), F32), copies],
        work,
    )
    (density,) = on_chip(
        near_terms_kernel,
        where,
        (
            *turned_gather(near_rows),
            *(partner_near, partner_far, near_a, near_b, far_a, far_b),
        ),
        [((2, half, n), BF16)],
        [
            full,
            pltpu.VMEM((2, half, n), F32),
            pltpu.VMEM((2, half, n), BF16),
            copies,
            copies,
        ],
        work,
        off_chip=(total,),
    )
    return density.reshape(three_index.shape)


def solution(mesh):
    torus = Mesh(
        mesh.devices.reshape(mesh.shape["virt"], mesh.shape["occ"] // 2, 2, X, C),
        ("v", "z", "h", "x", "c"),
    )
    placed = P(("x", "c"), ("z", "h"), "v")
    return jax.shard_map(
        on_device,
        mesh=torus,
        in_specs=(placed, P(("z", "h")), P("v")),
        out_specs=placed,
        check_vma=False,
    )
```

```python
import jax
import jax.numpy as jnp
from jax import lax
from jax.experimental import pallas as pl
from jax.experimental.pallas import tpu as pltpu
from jax.sharding import Mesh
from jax.sharding import PartitionSpec as P


SPIN_SCALE = 1.2
X, C = 4, 2
F32, BF16 = jnp.float32, jnp.bfloat16
NN = (((1,), (0,)), ((), ()))
NT = (((1,), (1,)), ((), ()))


def mm(left, right, dims):
    return lax.dot_general(left, right, dims, preferred_element_type=F32)


def on_chip(kernel, where, operands, results, scratch, flops, off_chip=()):
    vmem, hbm = (pl.BlockSpec(memory_space=m) for m in (pltpu.VMEM, pltpu.HBM))
    held = [pltpu.with_memory_space_constraint(v, pltpu.VMEM) for v in operands]
    far_away = [pltpu.with_memory_space_constraint(v, pltpu.HBM) for v in off_chip]
    return pl.pallas_call(
        kernel,
        in_specs=[pl.BlockSpec(memory_space=pltpu.SMEM)]
        + [hbm] * len(far_away)
        + [vmem] * len(held),
        out_specs=[hbm] * len(results),
        out_shape=[pltpu.HBM(*r) for r in results],
        scratch_shapes=scratch,
        compiler_params=pltpu.CompilerParams(vmem_limit_bytes=20 << 20),
        cost_estimate=pl.CostEstimate(flops=flops, bytes_accessed=flops // 1000, transcendentals=0),
    )(where, *far_away, *held)


def ring(axis, distance):
    size = lax.axis_size(axis)
    return [(i, (i + distance) % size) for i in range(size)]


def moved(value, axis, distance):
    return lax.ppermute(value, axis, ring(axis, distance))


def after(value, *events):
    return lax.optimization_barrier((value, *events))[0]


STRIP = 256


def add_products(core, first, lefts, rights, outs, ready, sent):
    part, n = ready.shape[3:]
    half = part * X

    def sending(j, number):
        columns = pl.ds(pl.multiple_of(j * STRIP, STRIP), STRIP)
        source = ready.at[number, :, :, :, columns]
        return pltpu.make_async_copy(source, outs[number].at[:, :, :, columns], sent.at[j, number])

    def step(j, carry):
        columns = pl.ds(pl.multiple_of(j * STRIP, STRIP), STRIP)
        for number, side in enumerate((1 - core, core)):
            rows = pl.ds(pl.multiple_of(side * half, 128), half)
            for place in range(2):
                product = mm(lefts[place][rows, :], rights[place][:, columns], NN)
                for k in range(X):
                    chunk = lax.rem(k - first + X, X)
                    ready[number, chunk, place, :, columns] = product[k * part : (k + 1) * part]
            sending(j, number).start()
        return carry

    lax.fori_loop(0, n // STRIP, step, 0)
    for j in range(n // STRIP):
        for number in range(2):
            sending(j, number).wait()


def turn(block, out):
    strip = 256

    def step(j, carry):
        part = pl.ds(pl.multiple_of(j * strip, strip), strip)
        out[part, :] = block[:, part].T
        return carry

    lax.fori_loop(0, block.shape[1] // strip, step, 0)


def far_pairs_kernel(where, own_high, behind, ahead, own_low, *refs):
    outs, lefts, (ready, sent) = refs[:2], refs[2:4], refs[4:]
    turn(own_high, lefts[0])
    turn(behind, lefts[1])
    add_products(where[1], 0, lefts, (ahead, own_low), outs, ready, sent)


def near_pairs_kernel(where, behind, partner, ahead, own, *refs):
    outs, lefts, (ready, sent) = refs[:2], refs[2:4], refs[4:]
    core, x = where[1], where[2]

    @pl.when(where[0] == 0)
    def _():
        turn(partner, lefts[0])
        turn(behind, lefts[1])
        add_products(core, x, lefts, (own, partner), outs, ready, sent)

    @pl.when(where[0] == 1)
    def _():
        turn(own, lefts[0])
        turn(partner, lefts[1])
        add_products(core, x, lefts, (partner, ahead), outs, ready, sent)


def copy_kernel(value, out):
    for k in range(value.shape[0]):
        out[k] = value[k]


def copied(value):
    table = pl.BlockSpec(memory_space=pltpu.SMEM)
    return pl.pallas_call(
        copy_kernel,
        in_specs=[table],
        out_specs=table,
        out_shape=jax.ShapeDtypeStruct(value.shape, value.dtype),
    )(value)


def pair_call(kernel, where, operands):
    half, n = operands[-1].shape
    shape = (X, 2, n // (X * C), n)
    scratch = [pltpu.VMEM((n, half), BF16)] * 2
    scratch += [pltpu.VMEM((2, *shape), F32), pltpu.SemaphoreType.DMA((n // STRIP, 2))]
    return on_chip(kernel, where, operands, [(shape, F32)] * 2, scratch, 4 * half * n * n)


def assemble(where, mine, other, full):
    part = mine.shape[2]
    core = where[1]
    for pieces, side in ((mine, core), (other, 1 - core)):
        for j in range(X):
            row = pl.multiple_of(side * (part * X) + j * part, 32)
            for place in range(2):
                full[place, pl.ds(row, part), :] = pieces[j, place]


STEP_ROWS = 256


def row_block(k):
    return pl.ds(pl.multiple_of(k * STEP_ROWS, STEP_ROWS), STEP_ROWS)


def far_terms_kernel(
    where, mine, other, ahead0, ahead1, behind0, behind1, out, full, ready, sent
):
    assemble(where, mine, other, full)
    steps = ahead0.shape[0] // STEP_ROWS

    def sending(k):
        rows = row_block(k)
        return pltpu.make_async_copy(ready.at[:, rows, :], out.at[:, rows, :], sent.at[k])

    def step(k, carry):
        rows = row_block(k)
        for place, (ahead, behind) in enumerate(((ahead0, behind0), (ahead1, behind1))):
            value = mm(ahead[rows, :], full[0], NT) + mm(behind[rows, :], full[1], NN)
            ready[place, rows, :] = value
        sending(k).start()
        return carry

    lax.fori_loop(0, steps, step, 0)
    for k in range(steps):
        sending(k).wait()


def assemble_turned(where, pieces, full):
    part = pieces[0].shape[1]
    core, x = where[1], where[2]
    for number, piece in enumerate(pieces):
        turn_by, other = number % X, number // X
        row = lax.rem(core + other, C) * (part * X) + lax.rem(x - turn_by + X, X) * part
        for place in range(2):
            full[place, pl.ds(pl.multiple_of(row, 32), part), :] = piece[place]


def near_terms_kernel(where, total, *refs):
    pieces, refs = refs[: X * C], refs[X * C :]
    partner_near, partner_far, near_a, near_b, far_a, far_b = refs[:6]
    out, full, loaded, ready, arrived, sent = refs[6:]
    steps = loaded.shape[1] // STEP_ROWS
    cuts = near_a.shape[0] // STEP_ROWS, far_a.shape[0] // STEP_ROWS

    def loading(k):
        rows = row_block(k)
        return pltpu.make_async_copy(total.at[:, rows, :], loaded.at[:, rows, :], arrived.at[k])

    def sending(k):
        rows = row_block(k)
        return pltpu.make_async_copy(ready.at[:, rows, :], out.at[:, rows, :], sent.at[k])

    for k in range(steps):
        loading(k).start()
    assemble_turned(where, pieces, full)

    def add(side, partner_dims, diagonal_dims):
        edges = sorted({0, *cuts, steps})
        for start, end in zip(edges, edges[1:]):
            sources = [
                (first, 0) if start < cut else (second, cut)
                for cut, first, second in zip(cuts, (near_a, far_a), (near_b, far_b))
            ]

            def step(number, carry, sources=sources):
                rows = row_block(number)
                loading(number).wait()
                for place, partner, (diagonal, offset) in (
                    (side, partner_near, sources[0]),
                    (1 - side, partner_far, sources[1]),
                ):
                    value = loaded[place, rows, :] + mm(partner[rows, :], full[0], partner_dims)
                    local = row_block(number - offset)
                    value = value + mm(diagonal[local, :], full[1], diagonal_dims)
                    ready[place, rows, :] = value.astype(ready.dtype)
                sending(number).start()
                return carry

            lax.fori_loop(start, end, step, 0)

    @pl.when(where[0] == 0)
    def _():
        add(0, NN, NT)

    @pl.when(where[0] == 1)
    def _():
        add(1, NT, NN)

    for k in range(steps):
        sending(k).wait()


def core_swap(value):
    return lax.ppermute(value, "c", [(0, 1), (1, 0)])


def exchanged(blocks):
    return lax.all_to_all(blocks, "x", 0, 0, tiled=True)


def summed_rows(paired):
    return jnp.sum(exchanged(paired).astype(F32), axis=0)


def turned_in(values):
    results = []
    for t, value in enumerate(values):
        results.append(moved(value, "x", t + 1))
    return results


def turned_sum(send, keep):
    other = core_swap(send)
    mine, *rest = (keep[t] + other[t] for t in range(X))
    rest = [r.astype(BF16) for r in rest]
    pieces = turned_in(rest)
    for piece in pieces:
        mine = mine + piece.astype(F32)
    return mine


def turned_gather(rows):
    pieces = [rows, *turned_in([rows] * (X - 1))]
    return pieces + [core_swap(p) for p in pieces]


def amplitude_rows(sums, left_levels, right_levels):
    denominator = left_levels[:, None] + right_levels[None, :]
    return (SPIN_SCALE * sums / denominator).astype(BF16)


def gathered(rows):
    mine = exchanged(jnp.broadcast_to(rows, (X, *rows.shape)))
    return mine, core_swap(mine)


def on_device(three_index, occupied_energy, virtual_energy):
    rows, _, n = three_index.shape
    half, quarter = rows // 2, rows // 4
    own = three_index.reshape(rows, n)
    h, c, x = lax.axis_index("h"), lax.axis_index("c"), lax.axis_index("x")
    where = jnp.stack([h, c, x]).astype(jnp.int32)
    even = h == 0
    zh = lax.axis_size("z") * 2
    swap_h = [(0, 1), (1, 0)]
    along_route = [(i, (i + (2 if i % 2 == 0 else -2)) % zh) for i in range(zh)]

    def ahead_of(value):
        return lax.ppermute(value, "z", ring("z", 1))

    def behind_of(value):
        return lax.ppermute(value, "z", ring("z", -1))

    def partner_of(value):
        return lax.ppermute(value, "h", swap_h)

    def along(value):
        return lax.ppermute(value, ("z", "h"), along_route)

    def energy(axis, route):
        return lax.ppermute(occupied_energy, axis, route)

    def cut(value, start, length):
        return lax.dynamic_slice_in_dim(value, start, length, 0)

    high = cut(own, half, half)
    low = cut(after(own, high), 0, half)
    far = cut(after(own, low), (1 - h) * half, half)
    near = cut(after(own, far), h * half, half)
    ahead1 = ahead_of(high)
    behind0 = behind_of(low)
    partner_near = partner_of(far)

    ahead0 = ahead_of(low)
    behind1 = behind_of(high)
    partner_far = partner_of(near)

    own_e = occupied_energy.astype(F32)
    ahead_e = energy("z", ring("z", 1))
    behind_e = energy("z", ring("z", -1))
    partner_e = energy("h", swap_h)
    diagonal_e = energy(("z", "h"), [(i, (i + (1 if i % 2 else -1)) % zh) for i in range(zh)])

    far_send, far_keep = pair_call(far_pairs_kernel, where, (high, behind0, ahead1, low))
    near_send, near_keep = pair_call(
        near_pairs_kernel, where, (behind0, partner_near, ahead1, near)
    )

    def facing(start):
        cuts = (v[start : start + quarter] for v in (behind0, ahead1))
        return jnp.where(even, *cuts)

    far_a = partner_of(facing(0))
    far_b = partner_of(facing(quarter))
    near_a = along(partner_near[:STEP_ROWS])
    near_b = along(cut(partner_near, STEP_ROWS, half - STEP_ROWS))

    paired = (far_keep + core_swap(far_send)).astype(BF16)
    far_sums = summed_rows(paired)
    near_sums = turned_sum(near_send, near_keep)
    ahead_e, behind_e, partner_e, diagonal_e = (
        after(e, paired).astype(F32) for e in (ahead_e, behind_e, partner_e, diagonal_e)
    )

    far_wire = far_sums.astype(BF16)
    from_ahead = ahead_of(far_wire[1])
    from_behind = behind_of(far_wire[0])
    near_wire = near_sums.astype(BF16)
    from_partner = partner_of(near_wire)
    from_along = along(near_wire[1])

    share = n // (X * C)
    my_levels = lax.dynamic_slice_in_dim(virtual_energy, c * (n // C) + x * share, share, 0)

    def levels(left_e, right_e):
        return my_levels - left_e, virtual_energy - right_e

    far_rows = jnp.stack(
        [
            amplitude_rows(far_sums[0] + from_ahead.astype(F32), *levels(own_e, ahead_e)),
            amplitude_rows(far_sums[1] + from_behind.astype(F32), *levels(behind_e, own_e)),
        ]
    )
    from_partner = after(from_partner, far_rows)
    near_rows = jnp.stack(
        [
            amplitude_rows(
                near_sums[0] + from_partner[0].astype(F32),
                *levels(jnp.where(even, partner_e, own_e), jnp.where(even, own_e, partner_e)),
            ),
            amplitude_rows(
                from_partner[1].astype(F32) + from_along.astype(F32),
                *levels(jnp.where(even, own_e, diagonal_e), jnp.where(even, diagonal_e, own_e)),
            ),
        ]
    )

    full = pltpu.VMEM((2, n, n), BF16)
    copies = pltpu.SemaphoreType.DMA((half // STEP_ROWS,))
    work = 8 * half * n * n
    (total,) = on_chip(
        far_terms_kernel,
        copied(where),
        (*gathered(far_rows), ahead0, ahead1, behind0, behind1),
        [((2, half, n), F32)],
        [full, pltpu.VMEM((2, half, n), F32), copies],
        work,
    )
    (density,) = on_chip(
        near_terms_kernel,
        where,
        (
            *turned_gather(near_rows),
            *(partner_near, partner_far, near_a, near_b, far_a, far_b),
        ),
        [((2, half, n), BF16)],
        [
            full,
            pltpu.VMEM((2, half, n), F32),
            pltpu.VMEM((2, half, n), BF16),
            copies,
            copies,
        ],
        work,
        off_chip=(total,),
    )
    return density.reshape(three_index.shape)


def solution(mesh):
    torus = Mesh(
        mesh.devices.reshape(mesh.shape["virt"], mesh.shape["occ"] // 2, 2, X, C),
        ("v", "z", "h", "x", "c"),
    )
    placed = P(("x", "c"), ("z", "h"), "v")
    return jax.shard_map(
        on_device,
        mesh=torus,
        in_specs=(placed, P(("z", "h")), P("v")),
        out_specs=placed,
        check_vma=False,
    )
```
